32 devices in a mesh: energy: 4 (over z), orb: 4 (over y, x), kpt: 2 (over core).
Axes of the slice: x: 2, y: 2, z: 4, core: 2. Of those that a mesh axis runs over, the one named last changes fastest.
Arguments:
- lesser: bfloat16 [2, 4, 16, 1, 512, 512], P(None, 'energy', 'kpt', None, None, 'orb'), may hold values from -6 to 6
- coupling: bfloat16 [2, 16, 512, 512], P(None, None, None, 'orb'), may hold values from -0.046875 to 0.046875
- transfer_map: int32 [16, 16], replicated, may hold values from 0 to 15, as said below
Outputs:
- sigma: bfloat16 [2, 4, 16, 1, 512, 512], P(None, None, 'kpt', None, 'energy', 'orb')
The draws below stay inside these ranges and needn't reach their ends.
Inputs may be any that keep to these rules, and one draw needn't show every extreme that they name: transfer_map[k, p] is the index of the momentum transfer k - p: each row and each column holds every number of 0 to 15 once.
All inputs are finite; a program needn't handle non-finite values.
Results may differ from the reference program's by a relative error of at most 0.001.
Values may be sent and summed in bfloat16 or wider, within the bound.
A program may use at most 128 MiB of HBM per device.

```python
import jax
import jax.numpy as jnp
from jax import lax

NO = 512
LAYERS = 1
K = 16
ENERGIES = 4


def draw_transfer_map(key, part):
    ranking = jax.random.permutation(jax.random.fold_in(key, 7), K).astype(jnp.int32)
    target_ids = jnp.arange(K, dtype=jnp.int32)
    shifts = (target_ids[:, None] - target_ids[None, :]) % K
    return ranking[shifts]


def shard_levels(stream_key, shape, shards, low, largest):
    def one(position, parts):
        draws = jax.random.uniform(jax.random.fold_in(jax.random.fold_in(stream_key, 6), position), (parts,), jnp.float32, low / len(shards), largest / len(shards))
        return jnp.repeat(jnp.exp(draws), shape[position] // parts).reshape((-1,) + (1,) * (len(shape) - position - 1))

    factor_of = one(*shards[0])
    for cut in shards[1:]:
        factor_of = factor_of * one(*cut)
    return factor_of


def normal_values(rng, shape, spread, bound, split=(), kind=jnp.bfloat16):
    result = jax.random.normal(rng, shape, jnp.float32) * spread
    if len(split) > 0:
        result = shard_levels(rng, shape, split, -0.22, 0.18) * result
    return jnp.clip(result, min=-bound, max=bound).astype(kind)


def setup_inputs(seed: int = 0) -> dict:
    key_of = jax.random.split(jax.random.key(seed), 4)
    return {
        "lesser": normal_values(key_of[0], (2, ENERGIES, K, LAYERS, NO, NO), 1.0, 6.0, ((1, 4), (2, 2), (5, 4))),
        "coupling": normal_values(key_of[1], (2, K, NO, NO), (2 * NO * K) ** -0.5, 0.046875, ((3, 4),)),
        "transfer_map": draw_transfer_map(jax.random.fold_in(key_of[3], 71), 0),
    }


def reference(lesser, coupling, transfer_map):
    real_green = lesser[0].astype(jnp.float32)
    imag_green = lesser[1].astype(jnp.float32)

    def per_target(target):
        selected = jnp.take(coupling, transfer_map[target], axis=1).astype(jnp.float32)
        real_out = jnp.einsum("eplrm,pmj->elrj", real_green, selected[0]) - jnp.einsum("eplrm,pmj->elrj", imag_green, selected[1])
        imag_out = jnp.einsum("eplrm,pmj->elrj", real_green, selected[1]) + jnp.einsum("eplrm,pmj->elrj", imag_green, selected[0])
        return jnp.stack([real_out, imag_out]).astype(jnp.bfloat16)

    stacked = lax.map(per_target, jnp.arange(K, dtype=jnp.int32))
    return jnp.transpose(stacked, (1, 2, 0, 3, 4, 5))
```

```python
import functools

import jax
import jax.numpy as jnp
from jax import lax
from jax.experimental import pallas as pl
from jax.experimental.pallas import tpu as pltpu
from jax.sharding import PartitionSpec as P

MESH = pl.DeviceIdType.MESH
X, Y, DA, DB, P0, PX, PY, PD = range(8)


def complex_terms(green, selected):
    real_out = jnp.einsum(
        "prm,tpmj->trj", green[0], selected[0], preferred_element_type=jnp.float32
    ) - jnp.einsum("prm,tpmj->trj", green[1], selected[1], preferred_element_type=jnp.float32)
    imag_out = jnp.einsum(
        "prm,tpmj->trj", green[0], selected[1], preferred_element_type=jnp.float32
    ) + jnp.einsum("prm,tpmj->trj", green[1], selected[0], preferred_element_type=jnp.float32)
    return (real_out, imag_out)


def per_device_general(lesser, coupling, transfer_map):
    regrouped = lax.all_to_all(lesser, "energy", split_axis=4, concat_axis=1, tiled=True)
    gathered = lax.all_gather(regrouped, "orb", axis=5, tiled=True)
    energies = gathered.shape[1]
    local_points = gathered.shape[2]
    layers = gathered.shape[3]
    tile = gathered.shape[4]
    width = gathered.shape[5]
    out_cols = coupling.shape[3]
    row_count = energies * layers * tile
    first_point = lax.axis_index("kpt") * local_points
    reordered = jnp.moveaxis(gathered, 2, 1).reshape(2, local_points, row_count, width)
    my_columns = lax.dynamic_slice_in_dim(transfer_map, first_point, local_points, 1)
    selected = jnp.take(coupling, my_columns, axis=1)
    real_out, imag_out = complex_terms(reordered, selected)
    mine = lax.psum_scatter(
        jnp.stack([real_out, imag_out], axis=1), "kpt", scatter_dimension=0, tiled=True
    )
    summed = jnp.moveaxis(mine, 1, 0)
    result = summed.astype(jnp.bfloat16).reshape(2, local_points, energies, layers, tile, out_cols)
    return jnp.moveaxis(result, 1, 2)


def kernel(nz, map_ref, lesser, coupling, out, g, u, acc, zsend, zrecv, send, recv, local_sem, u_sem):
    points = lesser.shape[2]
    width = lesser.shape[5]
    tile = g.shape[5]
    rows = nz * tile
    e = lax.axis_index("energy")
    o = lax.axis_index("orb")
    c = lax.axis_index("kpt")
    ox = o + 1 - 2 * lax.rem(o, 2)
    oy = lax.rem(o + 2, 4)
    od = 3 - o
    cp = 1 - c

    def to_energy(d):
        return lax.rem(e + d, nz)

    def from_energy(d):
        return lax.rem(e + nz - d, nz)

    def own_rows(s, z):
        return lesser.at[:, 0, s, 0, pl.ds(pl.multiple_of(z * tile, tile), tile), :]

    def z_copy(d, s, owner, target):
        return pltpu.make_async_remote_copy(
            src_ref=own_rows(s, target),
            dst_ref=g.at[c, o, :, s, owner],
            send_sem=zsend.at[d - 1, s],
            recv_sem=zrecv.at[d - 1, s],
            device_id={"energy": target},
            device_id_type=MESH,
        )

    def local_copy(s):
        return pltpu.make_async_copy(own_rows(s, e), g.at[c, o, :, s, e], local_sem.at[s])

    def move(kind, s, ref, target):
        return pltpu.make_async_remote_copy(
            src_ref=ref,
            dst_ref=ref,
            send_sem=send.at[kind, s],
            recv_sem=recv.at[kind, s],
            device_id=target,
            device_id_type=MESH,
        )

    def block(k, q, s):
        return g.at[k, q, :, s]

    def half(q, part, s):
        return g.at[c, q, part, s]

    to_x, to_y, to_peer = {"orb": ox}, {"orb": oy}, {"kpt": cp}

    def outgoing(s):
        return {
            X: move(X, s, block(c, o, s), to_x),
            Y: move(Y, s, block(c, o, s), to_y),
            P0: move(P0, s, block(c, o, s), to_peer),
            DA: move(DA, s, half(ox, 0, s), to_y),
            PX: move(PX, s, block(c, ox, s), to_peer),
            DB: move(DB, s, half(oy, 1, s), to_x),
            PY: move(PY, s, block(c, oy, s), to_peer),
            PD: move(PD, s, block(c, od, s), to_peer),
        }

    def incoming(s):
        return {
            X: move(X, s, block(c, ox, s), to_x),
            Y: move(Y, s, block(c, oy, s), to_y),
            DA: move(DA, s, half(od, 0, s), to_y),
            DB: move(DB, s, half(od, 1, s), to_x),
            P0: move(P0, s, block(cp, o, s), to_peer),
            PX: move(PX, s, block(cp, ox, s), to_peer),
            PY: move(PY, s, block(cp, oy, s), to_peer),
            PD: move(PD, s, block(cp, od, s), to_peer),
        }

    def locals_start(s, _):
        local_copy(s).start()
        return 0

    lax.fori_loop(0, points, locals_start, 0)
    u_copy = pltpu.make_async_copy(coupling, u, u_sem)
    u_copy.start()

    barrier = pltpu.get_barrier_semaphore()
    for d in range(1, nz):
        pl.semaphore_signal(barrier, inc=1, device_id={"energy": to_energy(d)}, device_id_type=MESH)
    for target in (to_x, to_y, to_peer):
        pl.semaphore_signal(barrier, inc=1, device_id=target, device_id_type=MESH)
    pl.semaphore_wait(barrier, nz - 1 + 3)

    def z_start(s, _):
        for d in range(1, nz):
            z_copy(d, s, e, to_energy(d)).start()
        return 0

    lax.fori_loop(0, points, z_start, 0)

    def clear(t, _):
        acc[t] = jnp.zeros(acc.shape[1:], acc.dtype)
        return 0

    lax.fori_loop(0, points, clear, 0)
    u_copy.wait()

    def multiply(chunks, s):
        def one(t, _):
            lhs, rhs = [], []
            for k, q in chunks:
                lhs.append(g[k, q, 0, s].reshape(rows, width))
                lhs.append(g[k, q, 1, s].reshape(rows, width))
                index = map_ref[c * points + t, k * points + s]
                at = pl.ds(pl.multiple_of(q * width, width), width)
                ur = u[0, index, at, :]
                ui = u[1, index, at, :]
                rhs.append(jnp.concatenate([ur, ui], axis=1))
                rhs.append(jnp.concatenate([-ui, ur], axis=1))
            acc[t] += jnp.dot(
                jnp.concatenate(lhs, axis=1),
                jnp.concatenate(rhs, axis=0),
                preferred_element_type=jnp.float32,
            )
            return 0

        lax.fori_loop(0, points, one, 0)

    def tick(s, _):
        @pl.when(s < points)
        def _():
            for d in range(1, nz):
                z_copy(d, s, from_energy(d), e).wait_recv()
            local_copy(s).wait()
            go = outgoing(s)
            for kind in (X, Y, P0):
                go[kind].start()

        @pl.when((s >= 1) & (s < points + 1))
        def _():
            r = s - 1
            come, go = incoming(r), outgoing(r)
            come[X].wait_recv()
            go[DA].start()
            go[PX].start()
            come[Y].wait_recv()
            go[DB].start()
            go[PY].start()

        @pl.when((s >= 2) & (s < points + 2))
        def _():
            r = s - 2
            come, go = incoming(r), outgoing(r)
            come[DA].wait_recv()
            come[DB].wait_recv()
            go[PD].start()

        @pl.when((s >= 1) & (s < points + 1))
        def _():
            r = s - 1
            incoming(r)[P0].wait_recv()
            multiply(((c, o), (cp, o)), r)
            multiply(((c, ox), (c, oy)), r)

        @pl.when((s >= 2) & (s < points + 2))
        def _():
            r = s - 2
            come = incoming(r)
            come[PX].wait_recv()
            come[PY].wait_recv()
            multiply(((cp, ox), (cp, oy)), r)

        @pl.when(s >= 3)
        def _():
            r = s - 3
            incoming(r)[PD].wait_recv()
            multiply(((c, od), (cp, od)), r)

        return 0

    lax.fori_loop(0, points + 3, tick, 0)

    def finish(t, _):
        for k in range(nz):
            for part in range(2):
                values = acc[t, k * tile : (k + 1) * tile, part * width : (part + 1) * width]
                out[part, k, t, 0] = values.astype(out.dtype)
        return 0

    lax.fori_loop(0, points, finish, 0)

    def drain(s, _):
        for d in range(1, nz):
            z_copy(d, s, e, to_energy(d)).wait_send()
        go = outgoing(s)
        for kind in range(8):
            go[kind].wait_send()
        return 0

    lax.fori_loop(0, points, drain, 0)


def per_device_fused(nz, lesser, coupling, transfer_map):
    points = lesser.shape[2]
    tile = lesser.shape[4] // nz
    width = lesser.shape[5]
    out_cols = coupling.shape[3]
    dma = pltpu.SemaphoreType.DMA
    return pl.pallas_call(
        functools.partial(kernel, nz),
        out_shape=jax.ShapeDtypeStruct((2, nz, points, 1, tile, out_cols), jnp.bfloat16),
        in_specs=[
            pl.BlockSpec(memory_space=pltpu.SMEM),
            pl.BlockSpec(memory_space=pl.ANY),
            pl.BlockSpec(memory_space=pl.ANY),
        ],
        out_specs=pl.BlockSpec(memory_space=pltpu.VMEM),
        scratch_shapes=[
            pltpu.VMEM((2, 4, 2, points, nz, tile, width), lesser.dtype),
            pltpu.VMEM(coupling.shape, coupling.dtype),
            pltpu.VMEM((points, nz * tile, 2 * out_cols), jnp.float32),
            dma((nz - 1, points)),
            dma((nz - 1, points)),
            dma((8, points)),
            dma((8, points)),
            dma((points,)),
            dma(()),
        ],
        compiler_params=pltpu.CompilerParams(
            collective_id=0, has_side_effects=True, vmem_limit_bytes=56 * 1024 * 1024
        ),
    )(transfer_map, lesser, coupling)


def solution(mesh):
    in_specs = (P(None, "energy", "kpt", None, None, "orb"), P(None, None, None, "orb"), P())
    out_specs = P(None, None, "kpt", None, "energy", "orb")
    nz = mesh.shape["energy"]

    def per_device(lesser, coupling, transfer_map):
        shape = lesser.shape
        fused = (
            mesh.shape["orb"] == 4
            and mesh.shape["kpt"] == 2
            and nz > 1
            and shape[1] == 1
            and shape[3] == 1
            and shape[5] == coupling.shape[3] == 128
            and shape[4] == nz * 128
        )
        if fused:
            return per_device_fused(nz, lesser, coupling, transfer_map)
        return per_device_general(lesser, coupling, transfer_map)

    return jax.shard_map(
        per_device, mesh=mesh, in_specs=in_specs, out_specs=out_specs, check_vma=False
    )
```

```python
import functools

import jax
import jax.numpy as jnp
from jax import lax
from jax.experimental import pallas as pl
from jax.experimental.pallas import tpu as pltpu
from jax.sharding import PartitionSpec as P

MESH = pl.DeviceIdType.MESH
DA, DB, P0, PX, PY, PD = range(6)
AHEAD = 1


def complex_terms(green, selected):
    real_out = jnp.einsum(
        "prm,tpmj->trj", green[0], selected[0], preferred_element_type=jnp.float32
    ) - jnp.einsum("prm,tpmj->trj", green[1], selected[1], preferred_element_type=jnp.float32)
    imag_out = jnp.einsum(
        "prm,tpmj->trj", green[0], selected[1], preferred_element_type=jnp.float32
    ) + jnp.einsum("prm,tpmj->trj", green[1], selected[0], preferred_element_type=jnp.float32)
    return (real_out, imag_out)


def per_device_general(lesser, coupling, transfer_map):
    regrouped = lax.all_to_all(lesser, "energy", split_axis=4, concat_axis=1, tiled=True)
    gathered = lax.all_gather(regrouped, "orb", axis=5, tiled=True)
    energies = gathered.shape[1]
    local_points = gathered.shape[2]
    layers = gathered.shape[3]
    tile = gathered.shape[4]
    width = gathered.shape[5]
    out_cols = coupling.shape[3]
    row_count = energies * layers * tile
    first_point = lax.axis_index("kpt") * local_points
    reordered = jnp.moveaxis(gathered, 2, 1).reshape(2, local_points, row_count, width)
    my_columns = lax.dynamic_slice_in_dim(transfer_map, first_point, local_points, 1)
    selected = jnp.take(coupling, my_columns, axis=1)
    real_out, imag_out = complex_terms(reordered, selected)
    mine = lax.psum_scatter(
        jnp.stack([real_out, imag_out], axis=1), "kpt", scatter_dimension=0, tiled=True
    )
    summed = jnp.moveaxis(mine, 1, 0)
    result = summed.astype(jnp.bfloat16).reshape(2, local_points, energies, layers, tile, out_cols)
    return jnp.moveaxis(result, 1, 2)


def kernel(nz, map_ref, lesser, coupling, out, g, u, acc, zsend, zrecv, osend, orecv, send, recv, local_sem, u_sem):
    points = lesser.shape[2]
    width = lesser.shape[5]
    tile = g.shape[5]
    rows = nz * tile
    e = lax.axis_index("energy")
    o = lax.axis_index("orb")
    c = lax.axis_index("kpt")
    ox = o + 1 - 2 * lax.rem(o, 2)
    oy = lax.rem(o + 2, 4)
    od = 3 - o
    cp = 1 - c

    def to_energy(d):
        return lax.rem(e + d, nz)

    def from_energy(d):
        return lax.rem(e + nz - d, nz)

    def own_rows(s, z):
        return lesser.at[:, 0, s, 0, pl.ds(pl.multiple_of(z * tile, tile), tile), :]

    def z_copy(d, s, owner, target):
        return pltpu.make_async_remote_copy(
            src_ref=own_rows(s, target),
            dst_ref=g.at[c, o, :, s, owner],
            send_sem=zsend.at[d - 1, s],
            recv_sem=zrecv.at[d - 1, s],
            device_id={"energy": target},
            device_id_type=MESH,
        )

    def local_copy(s):
        return pltpu.make_async_copy(own_rows(s, e), g.at[c, o, :, s, e], local_sem.at[s])

    def move(kind, s, ref, target):
        return pltpu.make_async_remote_copy(
            src_ref=ref,
            dst_ref=ref,
            send_sem=send.at[kind, s],
            recv_sem=recv.at[kind, s],
            device_id=target,
            device_id_type=MESH,
        )

    def own_copy(way, d, s):
        owner = from_energy(d)
        tile_ref = g.at[c, o, :, s, owner]
        return pltpu.make_async_remote_copy(
            src_ref=own_rows(s, e) if d == 0 else tile_ref,
            dst_ref=tile_ref,
            send_sem=osend.at[way, d, s],
            recv_sem=orecv.at[way, d, s],
            device_id=(to_x, to_y)[way],
            device_id_type=MESH,
        )

    def wait_own(way, s):
        for d in range(nz):
            tile_ref = g.at[c, (ox, oy)[way], :, s, from_energy(d)]
            pltpu.make_async_remote_copy(
                src_ref=tile_ref,
                dst_ref=tile_ref,
                send_sem=osend.at[way, d, s],
                recv_sem=orecv.at[way, d, s],
                device_id=(to_x, to_y)[way],
                device_id_type=MESH,
            ).wait_recv()

    def block(k, q, s):
        return g.at[k, q, :, s]

    def half(q, part, s):
        return g.at[c, q, part, s]

    to_x, to_y, to_peer = {"orb": ox}, {"orb": oy}, {"kpt": cp}

    def outgoing(kind, s):
        refs = {
            P0: lambda: block(c, o, s),
            DA: lambda: half(ox, 0, s),
            PX: lambda: block(c, ox, s),
            DB: lambda: half(oy, 1, s),
            PY: lambda: block(c, oy, s),
            PD: lambda: block(c, od, s),
        }
        return move(kind, s, refs[kind](), {DA: to_y, DB: to_x}.get(kind, to_peer))

    def incoming(kind, s):
        refs = {
            DA: lambda: half(od, 0, s),
            DB: lambda: half(od, 1, s),
            P0: lambda: block(cp, o, s),
            PX: lambda: block(cp, ox, s),
            PY: lambda: block(cp, oy, s),
            PD: lambda: block(cp, od, s),
        }
        return move(kind, s, refs[kind](), {DA: to_y, DB: to_x}.get(kind, to_peer))

    def locals_start(s, _):
        local_copy(s).start()
        return 0

    lax.fori_loop(0, points, locals_start, 0)
    u_copy = pltpu.make_async_copy(coupling, u, u_sem)
    u_copy.start()

    barrier = pltpu.get_barrier_semaphore()
    for d in range(1, nz):
        pl.semaphore_signal(barrier, inc=1, device_id={"energy": to_energy(d)}, device_id_type=MESH)
    for target in (to_x, to_y, to_peer):
        pl.semaphore_signal(barrier, inc=1, device_id=target, device_id_type=MESH)
    pl.semaphore_wait(barrier, nz - 1 + 3)

    def z_start(s, _):
        for d in range(1, nz):
            z_copy(d, s, e, to_energy(d)).start()
        own_copy(0, 0, s).start()
        own_copy(1, 0, s).start()
        return 0

    lax.fori_loop(0, points, z_start, 0)

    def clear(t, _):
        acc[t] = jnp.zeros(acc.shape[1:], acc.dtype)
        return 0

    lax.fori_loop(0, points, clear, 0)
    u_copy.wait()

    def multiply(chunks, s):
        def one(t, _):
            lhs, rhs = [], []
            for k, q in chunks:
                lhs.append(g[k, q, 0, s].reshape(rows, width))
                lhs.append(g[k, q, 1, s].reshape(rows, width))
                index = map_ref[c * points + t, k * points + s]
                at = pl.ds(pl.multiple_of(q * width, width), width)
                ur = u[0, index, at, :]
                ui = u[1, index, at, :]
                rhs.append(jnp.concatenate([ur, ui], axis=1))
                rhs.append(jnp.concatenate([-ui, ur], axis=1))
            acc[t] += jnp.dot(
                jnp.concatenate(lhs, axis=1),
                jnp.concatenate(rhs, axis=0),
                preferred_element_type=jnp.float32,
            )
            return 0

        lax.fori_loop(0, points, one, 0, unroll=True)

    def lagged(s, lag):
        return pl.when((s >= lag) & (s < points + lag))

    def tick(s, _):
        @lagged(s, 0)
        def _():
            for d in range(1, nz):
                z_copy(d, s, from_energy(d), e).wait_recv()
                own_copy(0, d, s).start()
                own_copy(1, d, s).start()
            local_copy(s).wait()
            outgoing(P0, s).start()

        @lagged(s, AHEAD)
        def _():
            r = s - AHEAD
            wait_own(0, r)
            outgoing(DA, r).start()
            outgoing(PX, r).start()
            wait_own(1, r)
            outgoing(DB, r).start()
            outgoing(PY, r).start()

        @lagged(s, AHEAD + 1)
        def _():
            r = s - AHEAD - 1
            incoming(DA, r).wait_recv()
            incoming(DB, r).wait_recv()
            outgoing(PD, r).start()

        @lagged(s, AHEAD)
        def _():
            r = s - AHEAD
            incoming(P0, r).wait_recv()
            multiply(((c, o), (cp, o)), r)
            multiply(((c, ox), (c, oy)), r)

        @lagged(s, AHEAD + 1)
        def _():
            r = s - AHEAD - 1
            incoming(PX, r).wait_recv()
            incoming(PY, r).wait_recv()
            multiply(((cp, ox), (cp, oy)), r)

        @lagged(s, AHEAD + 2)
        def _():
            r = s - AHEAD - 2
            incoming(PD, r).wait_recv()
            multiply(((c, od), (cp, od)), r)

        return 0

    lax.fori_loop(0, points + AHEAD + 2, tick, 0)

    def finish(t, _):
        for k in range(nz):
            for part in range(2):
                values = acc[t, k * tile : (k + 1) * tile, part * width : (part + 1) * width]
                out[part, k, t, 0] = values.astype(out.dtype)
        return 0

    lax.fori_loop(0, points, finish, 0)

    def drain(s, _):
        for d in range(1, nz):
            z_copy(d, s, e, to_energy(d)).wait_send()
        for d in range(nz):
            own_copy(0, d, s).wait_send()
            own_copy(1, d, s).wait_send()
        for kind in range(6):
            outgoing(kind, s).wait_send()
        return 0

    lax.fori_loop(0, points, drain, 0)


def per_device_fused(nz, lesser, coupling, transfer_map):
    points = lesser.shape[2]
    tile = lesser.shape[4] // nz
    width = lesser.shape[5]
    out_cols = coupling.shape[3]
    dma = pltpu.SemaphoreType.DMA
    return pl.pallas_call(
        functools.partial(kernel, nz),
        out_shape=jax.ShapeDtypeStruct((2, nz, points, 1, tile, out_cols), jnp.bfloat16),
        in_specs=[
            pl.BlockSpec(memory_space=pltpu.SMEM),
            pl.BlockSpec(memory_space=pl.ANY),
            pl.BlockSpec(memory_space=pl.ANY),
        ],
        out_specs=pl.BlockSpec(memory_space=pltpu.VMEM),
        scratch_shapes=[
            pltpu.VMEM((2, 4, 2, points, nz, tile, width), lesser.dtype),
            pltpu.VMEM(coupling.shape, coupling.dtype),
            pltpu.VMEM((points, nz * tile, 2 * out_cols), jnp.float32),
            dma((nz - 1, points)),
            dma((nz - 1, points)),
            dma((2, nz, points)),
            dma((2, nz, points)),
            dma((6, points)),
            dma((6, points)),
            dma((points,)),
            dma(()),
        ],
        compiler_params=pltpu.CompilerParams(
            collective_id=0, has_side_effects=True, vmem_limit_bytes=56 * 1024 * 1024
        ),
    )(transfer_map, lesser, coupling)


def solution(mesh):
    in_specs = (P(None, "energy", "kpt", None, None, "orb"), P(None, None, None, "orb"), P())
    out_specs = P(None, None, "kpt", None, "energy", "orb")
    nz = mesh.shape["energy"]

    def per_device(lesser, coupling, transfer_map):
        shape = lesser.shape
        fused = (
            mesh.shape["orb"] == 4
            and mesh.shape["kpt"] == 2
            and nz > 1
            and shape[1] == 1
            and shape[3] == 1
            and shape[5] == coupling.shape[3] == 128
            and shape[4] == nz * 128
        )
        if fused:
            return per_device_fused(nz, lesser, coupling, transfer_map)
        return per_device_general(lesser, coupling, transfer_map)

    return jax.shard_map(
        per_device, mesh=mesh, in_specs=in_specs, out_specs=out_specs, check_vma=False
    )
```
